32 devices in a mesh: win: 2 (over y), dx: 4 (over z), dy: 2 (over x), dz: 2 (over core).
Axes of the slice: x: 2, y: 2, z: 4, core: 2. Of those that a mesh axis runs over, the one named last changes fastest.
Arguments:
- fraction: float32 [3, 8, 2, 2, 768], P(None, ('win', 'dx'), 'dy', 'dz'), parts along dimension 1, may hold values from 0 to 1
- atom_type: int32 [8, 2, 2, 768], P(('win', 'dx'), 'dy', 'dz'), parts along dimension 0, may hold values from 0 to 31
- perturbed: int32 [8, 2, 2, 768], P(('win', 'dx'), 'dy', 'dz'), parts along dimension 0, may hold values from 0 to 1
- leaving: int32 [8, 2, 2, 2, 16], P(('win', 'dx'), 'dy', 'dz'), parts along dimension 0, may hold values from 0 to 767, as said below
- neighbours: int32 [8, 2, 2, 6, 16], P(('win', 'dx'), 'dy', 'dz'), parts along dimension 0, may hold values from 0 to 161, as said below
- counts: int32 [8, 2, 2, 6], P(('win', 'dx'), 'dy', 'dz'), parts along dimension 0, may hold values from 1 to 16, as said below
- sigma_table: float32 [32], replicated, may hold values from 0.8 to 1.2
- depth_table: float32 [32], replicated, may hold values from 0.002 to 0.03
- charge_table: float32 [32], replicated, may hold values from -1 to 1
- domain_edge: float32 [3], replicated, may hold values from 1 to 1.12
- coupling: float32 [2], P('win'), parts along dimension 0, may hold values from 0.1 to 0.9
Outputs:
- forces: float32 [3, 8, 2, 2, 768], P(None, ('win', 'dx'), 'dy', 'dz'), parts along dimension 1
- energy: float32 [2], P('win'), parts along dimension 0
- dhdl: float32 [2], P('win'), parts along dimension 0
The draws below stay inside these ranges and needn't reach their ends.
There are 2 independent parts, one for each index of `win`. The reference program is written for one: setup_inputs(seed, part) draws one part's arguments, and reference() takes and returns one part's arrays. A program takes and returns all parts, laid end to end along the dimension named above; an argument that names none is the same for every part. Nothing has to cross between parts.
Inputs may be any that keep to these rules, and one draw needn't show every extreme that they name: `leaving`: each domain lists 2 * 16 distinct slots: the first 16 leave toward the next domain, the last 16 toward the previous one. `neighbours`: each list holds 16 distinct ghost block numbers; entries at or past the block's count are valid numbers and are not used. `counts`: some block lists exactly 16 blocks in every draw.
All inputs are finite; a program needn't handle non-finite values.
Results may differ from the reference program's by a relative error of at most 0.0003.
Values sent between devices are 32-bit elements; how exact they have to be, the bound alone decides.
No kernel may reach another device: no remote copies, remote signals or barrier semaphores. Data moves between devices by JAX's collectives and lax.ppermute only.
A program may use at most 64 MiB of HBM per device.

```python
import math
import jax
import jax.numpy as jnp
from jax import lax

ATOMS_DEV = 768
NB = 16
MIG = 16
NTYPES = 32
NATOMS = 12288
N_DX = 4
N_DY = 2
N_DZ = 2


def draw_perturbed(key, part):
    shape = (N_DX, N_DY, N_DZ, ATOMS_DEV)
    position_x = jnp.arange(N_DX, dtype=jnp.int32)[:, None, None, None]
    threshold = 10 + 20 * position_x // max(N_DX - 1, 1)
    values = jax.random.randint(key, shape, 0, 100, dtype=jnp.int32)
    return (values < threshold).astype(jnp.int32)


def draw_leaving(key, part):
    shape = (N_DX, N_DY, N_DZ, ATOMS_DEV)
    scores = jax.random.randint(key, shape, 0, 2 ** 16, dtype=jnp.int32) * ATOMS_DEV + jnp.arange(ATOMS_DEV, dtype=jnp.int32)
    order = jnp.argsort(scores, axis=-1, stable=True).astype(jnp.int32)
    return order[..., :2 * MIG].reshape(N_DX, N_DY, N_DZ, 2, MIG)


def draw_neighbours(key, part):
    ghost_blocks = 27 * (ATOMS_DEV // 128)
    shape = (N_DX, N_DY, N_DZ, ATOMS_DEV // 128, ghost_blocks)
    scores = jax.random.randint(key, shape, 0, 2 ** 16, dtype=jnp.int32) * ghost_blocks + jnp.arange(ghost_blocks, dtype=jnp.int32)
    order = jnp.argsort(scores, axis=-1, stable=True).astype(jnp.int32)
    return order[..., :NB]


def draw_counts(key, part):
    shape = (N_DX, N_DY, N_DZ, ATOMS_DEV // 128)
    values = jax.random.randint(key, shape, 1, NB + 1, dtype=jnp.int32)
    return values.at[0, 0, 0, 0].set(NB)


def touch_ends(array, key, smallest, top_value):
    longest = array.shape.index(max(array.shape))
    spots = []
    for shift in (0, 1):
        where = [jax.random.randint(jax.random.fold_in(key, axis), (), 0, length) for axis, length in enumerate(array.shape)]
        where[longest] = (where[longest] + shift) % array.shape[longest]
        spots.append(tuple(where))
    return array.at[spots[0]].set(smallest).at[spots[1]].set(top_value)


def levels(own_key, extent, cuts, least, high):
    factor_of, own = 1.0, jax.random.fold_in(own_key, 6)
    for dim, parts in cuts:
        steps = jnp.exp(jax.random.uniform(jax.random.fold_in(own, dim), (parts,), jnp.float32, least / len(cuts), high / len(cuts)))
        factor_of = factor_of * jnp.repeat(steps, extent[dim] // parts).reshape([-1 if axis == dim else 1 for axis in range(len(extent))])
    return factor_of


def setup_inputs(seed: int = 0, part: int = 0) -> dict:
    seeds = jax.random.split(jax.random.key(seed), 12)
    part_splits = jax.random.split(jax.random.fold_in(seeds[11], part), 12)
    fraction = jnp.clip(1.0 * jax.random.uniform(part_splits[0], (3, N_DX, N_DY, N_DZ, ATOMS_DEV), jnp.float32) ** levels(part_splits[0], (3, N_DX, N_DY, N_DZ, ATOMS_DEV), ((1, 4), (2, 2), (3, 2)), -0.2, 0.2), 0.0, 1.0)
    atom_type = touch_ends(jax.random.randint(part_splits[1], (N_DX, N_DY, N_DZ, ATOMS_DEV), 0, NTYPES), jax.random.fold_in(part_splits[1], 1), 0, NTYPES - 1).astype(jnp.int32)
    perturbed = draw_perturbed(jax.random.fold_in(jax.random.fold_in(seeds[11], part), 71), part)
    leaving = draw_leaving(jax.random.fold_in(jax.random.fold_in(seeds[11], part), 71), part)
    neighbours = draw_neighbours(jax.random.fold_in(jax.random.fold_in(seeds[11], part), 71), part)
    counts = draw_counts(jax.random.fold_in(jax.random.fold_in(seeds[11], part), 71), part)
    sigma_table = jnp.clip(jnp.exp(jax.random.uniform(seeds[6], (NTYPES,), jnp.float32, math.log(0.8), math.log(1.2))), 0.8, 1.2)
    depth_table = jnp.clip(jnp.exp(jax.random.uniform(seeds[7], (NTYPES,), jnp.float32, math.log(0.002), math.log(0.03))), 0.002, 0.03)
    charge_table = jnp.clip(jax.random.uniform(seeds[8], (NTYPES,), jnp.float32, -1.0, 1.0), -1.0, 1.0)
    domain_edge = jnp.clip(jax.random.uniform(seeds[9], (3,), jnp.float32, 1.0, 1.12), 1.0, 1.12)
    coupling = jnp.clip(jax.random.uniform(part_splits[10], (1,), jnp.float32, 0.1, 0.9), 0.1, 0.9)
    return {"fraction": fraction, "atom_type": atom_type, "perturbed": perturbed, "leaving": leaving, "neighbours": neighbours, "counts": counts, "sigma_table": sigma_table, "depth_table": depth_table, "charge_table": charge_table, "domain_edge": domain_edge, "coupling": coupling}


soft_base = 0.3
soft_alpha = 0.5
charge_base = 0.3
charge_alpha = 0.5
coulomb = 0.1

def lookup(table_row, type_ids):
    onehot = type_ids[None, :] == jnp.arange(table_row.shape[0], dtype=jnp.int32)[:, None]
    return lax.optimization_barrier(jnp.sum(jnp.where(onehot, table_row[:, None], jnp.float32(0.0)), axis=0))

def pair_block(own_block, other_blocks, live_pairs, coupling_value):
    separation = own_block[0:3][None, :, :, None] - other_blocks[:, 0:3][:, :, None, :]
    radius_sq = lax.optimization_barrier(jnp.sum(separation * separation, axis=1))
    sigma_pair = 0.5 * (own_block[3][None, :, None] + other_blocks[:, 3][:, None, :])
    depth_pair = jnp.sqrt(own_block[4][None, :, None] * other_blocks[:, 4][:, None, :])
    charges = own_block[5][None, :, None] * other_blocks[:, 5][:, None, :]
    flagged = jnp.maximum(own_block[6][None, :, None], other_blocks[:, 6][:, None, :])
    scaled = coupling_value * flagged
    sigma_two = sigma_pair * sigma_pair
    sigma_six = sigma_two * sigma_two * sigma_two
    soft_six = sigma_six * (soft_base + soft_alpha * scaled) + radius_sq * radius_sq * radius_sq
    soft_two = charge_base + charge_alpha * scaled + radius_sq
    inverse_six = 1.0 / soft_six
    energy_lj = 4.0 * depth_pair * (sigma_six * sigma_six * inverse_six * inverse_six - sigma_six * inverse_six)
    grad_six = 4.0 * depth_pair * (sigma_six * inverse_six * inverse_six - 2.0 * sigma_six * sigma_six * inverse_six * inverse_six * inverse_six)
    energy_coul = coulomb * charges * lax.rsqrt(soft_two)
    grad_two = -0.5 * energy_coul / soft_two
    weight = 1.0 - scaled
    total_pair = energy_lj + energy_coul
    pair_energy = jnp.sum(weight * total_pair * live_pairs)
    pair_dhdl = jnp.sum(flagged * (-total_pair + weight * (grad_six * sigma_six * soft_alpha + grad_two * charge_alpha)) * live_pairs)
    force_scale = -weight * (6.0 * radius_sq * radius_sq * grad_six + 2.0 * grad_two) * live_pairs
    forces = lax.optimization_barrier(jnp.sum(force_scale[:, None] * separation, axis=(0, 3)))
    return (forces, pair_energy, pair_dhdl)

def block_terms(ghost_rows, listed_blocks, list_count, block_id, block_total, coupling_value):
    centre = 13 * block_total + block_id
    own_block = lax.dynamic_index_in_dim(ghost_rows, centre, 0, keepdims=False)
    other_blocks = jnp.take(ghost_rows, listed_blocks, axis=0)
    valid_slot = (jnp.arange(listed_blocks.shape[0], dtype=jnp.int32) < list_count).astype(jnp.float32)
    is_self = (listed_blocks == centre).astype(jnp.float32)[:, None, None] * jnp.eye(128, dtype=jnp.float32)[None]
    live_pairs = valid_slot[:, None, None] * (1.0 - is_self)
    return pair_block(own_block, other_blocks, live_pairs, coupling_value)

def reference(fraction, atom_type, perturbed, leaving, neighbours, counts, sigma_table, depth_table, charge_table, domain_edge, coupling):
    domains = N_DX * N_DY * N_DZ
    block_total = ATOMS_DEV // 128
    spacing = float(ATOMS_DEV) ** (1.0 / 3.0)
    type_ids = atom_type.reshape(-1)
    payload = jnp.concatenate([fraction.reshape(3, domains, ATOMS_DEV), lookup(sigma_table, type_ids).reshape(1, domains, ATOMS_DEV), lookup(depth_table, type_ids).reshape(1, domains, ATOMS_DEV), lookup(charge_table, type_ids).reshape(1, domains, ATOMS_DEV), perturbed.reshape(1, domains, ATOMS_DEV).astype(jnp.float32)], axis=0)
    leave_slots = leaving.reshape(domains, 2, MIG)
    upward = jnp.take_along_axis(payload, leave_slots[None, :, 0, :], axis=2)
    downward = jnp.take_along_axis(payload, leave_slots[None, :, 1, :], axis=2)
    shift_x = jnp.zeros((7, 1, 1), jnp.float32).at[0].set(1.0)
    from_below = jnp.roll(upward.reshape(7, N_DX, N_DY * N_DZ, MIG), 1, axis=1).reshape(7, domains, MIG) - shift_x
    from_above = jnp.roll(downward.reshape(7, N_DX, N_DY * N_DZ, MIG), -1, axis=1).reshape(7, domains, MIG) + shift_x

    def place(block_rows, down_slots, up_slots, lower_rows, upper_rows):
        return block_rows.at[:, down_slots].set(lower_rows).at[:, up_slots].set(upper_rows)
    moved = jax.vmap(place, in_axes=(1, 0, 0, 1, 1), out_axes=1)(payload, leave_slots[:, 1], leave_slots[:, 0], from_below, from_above)
    moved_grid = moved.reshape(7, N_DX, N_DY, N_DZ, ATOMS_DEV)
    list_flat = neighbours.reshape(domains, block_total, NB)
    count_flat = counts.reshape(domains, block_total)
    coupling_value = coupling[0]

    def one_domain(flat_id):
        index_x = flat_id // (N_DY * N_DZ)
        index_y = flat_id // N_DZ % N_DY
        index_z = flat_id % N_DZ
        pieces = []
        for step_x in range(3):
            for step_y in range(3):
                for step_z in range(3):
                    neighbour_rows = moved_grid[:, (index_x + step_x - 1) % N_DX, (index_y + step_y - 1) % N_DY, (index_z + step_z - 1) % N_DZ]
                    position = jnp.stack([(neighbour_rows[0] + jnp.float32(step_x - 1)) * domain_edge[0] * spacing, (neighbour_rows[1] + jnp.float32(step_y - 1)) * domain_edge[1] * spacing, (neighbour_rows[2] + jnp.float32(step_z - 1)) * domain_edge[2] * spacing], axis=0)
                    pieces.append(jnp.concatenate([position, neighbour_rows[3:]], axis=0))
        ghost_rows = jnp.stack(pieces, 0).reshape(27, 7, block_total, 128).transpose(0, 2, 1, 3).reshape(27 * block_total, 7, 128)
        listed = list_flat[flat_id]
        listed_count = count_flat[flat_id]

        def one_block(block_id):
            return block_terms(ghost_rows, listed[block_id], listed_count[block_id], block_id, block_total, coupling_value)
        forces, energies, dhdls = lax.map(one_block, jnp.arange(block_total, dtype=jnp.int32))
        return (forces.transpose(1, 0, 2).reshape(3, ATOMS_DEV), jnp.sum(energies), jnp.sum(dhdls))
    forces, energies, dhdls = lax.map(one_domain, jnp.arange(domains, dtype=jnp.int32))
    forces = forces.transpose(1, 0, 2).reshape(3, N_DX, N_DY, N_DZ, ATOMS_DEV)
    energy = (0.5 * jnp.sum(energies) / jnp.float32(NATOMS)).reshape(1)
    dhdl = (0.5 * jnp.sum(dhdls) / jnp.float32(NATOMS)).reshape(1)
    return (forces, energy, dhdl)
```

```python
import functools

import jax
import jax.numpy as jnp
from jax import lax
from jax.experimental import pallas as pl
from jax.experimental.pallas import tpu as pltpu
from jax.sharding import PartitionSpec as P

soft_base = 0.3
soft_alpha = 0.5
charge_base = 0.3
charge_alpha = 0.5
coulomb = 0.1
LANES = 128
SUB = 8


def ring(count, by):
    return [((i + by) % count, i) for i in range(count)]


def grid_ring(count_y, count_z, by_y, by_z):
    route = []
    for y in range(count_y):
        for z in range(count_z):
            source = ((y + by_y) % count_y) * count_z + (z + by_z) % count_z
            route.append((source, y * count_z + z))
    return route


def gather_lanes(rows, lanes):
    return jnp.take_along_axis(rows, lanes, axis=1, mode="promise_in_bounds")


def pack_kernel(blocks, width, fraction, kind, flag, leaving, out, slab):
    slab[...] = jnp.zeros(slab.shape, jnp.float32)
    slab[0 : 3 * blocks, :] = fraction[...]
    slab[3 * blocks : 4 * blocks, :] = kind[...].astype(jnp.float32)
    slab[4 * blocks : 5 * blocks, :] = flag[...].astype(jnp.float32)
    head = slab.shape[0] - 2 * SUB
    slab[head : head + 1, 0:width] = leaving[...].astype(jnp.float32)
    slots = jnp.broadcast_to(slab[head : head + 1, :], (SUB, LANES)).astype(jnp.int32)
    lane = slots & (LANES - 1)
    block = slots >> 7
    here = lax.broadcasted_iota(jnp.int32, (SUB, LANES), 0) == block
    for k in range(5):
        picked = gather_lanes(slab[k * blocks : k * blocks + SUB, :], lane)
        picked = jnp.sum(jnp.where(here, picked, 0.0), axis=0, keepdims=True)
        slab[head + SUB + k : head + SUB + k + 1, :] = picked
    out[...] = slab[...]


def migrate_kernel(blocks, mig, below2, below, own, above, above2, out):
    pad = own.shape[0] - 2 * SUB
    tail = pad + SUB
    leavers = [
        below2[...],
        below[tail : tail + SUB, :],
        own[tail : tail + SUB, :],
        above[tail : tail + SUB, :],
        above2[...],
    ]
    lane = lax.broadcasted_iota(jnp.int32, (SUB, LANES), 1)
    row = lax.broadcasted_iota(jnp.int32, (SUB, LANES), 0)
    place = row * LANES + lane
    shift = jnp.where(row == 0, 1.0, 0.0)
    for d, base in enumerate((below, own, above)):
        slots = jnp.broadcast_to(base[pad : pad + 1, :], (SUB, LANES)).astype(jnp.int32)
        from_above = pltpu.roll(leavers[d + 2], LANES - mig, 1) + shift
        from_below = pltpu.roll(leavers[d], mig, 1) - shift
        incoming = jnp.where(lane < mig, from_above, from_below)
        origin = jnp.full((SUB, LANES), -1, jnp.int32)
        for m in range(2 * mig):
            spot = jnp.broadcast_to(slots[:, m : m + 1], (SUB, LANES))
            origin = jnp.where(place == spot, m, origin)
        arrives = origin >= 0
        source = jnp.maximum(origin, 0)
        for k in range(5):
            fresh = gather_lanes(jnp.broadcast_to(incoming[k : k + 1, :], (SUB, LANES)), source)
            held = base[k * blocks : k * blocks + SUB, :]
            kept = jnp.where(arrives, fresh, held)
            start = d * pad + k * blocks
            out[start : start + blocks, :] = kept[0:blocks]


def newton_reciprocal(x):
    guess = pl.reciprocal(x, approx=True)
    return guess * (2.0 - x * guess)


def pair_kernel(
    blocks, spacing, images, listed, counts, edge, coupling, sigma_t, depth_t, charge_t, *refs
):
    columns = refs[: max(c for c, _ in images) + 1]
    forces, sums = refs[len(columns) : len(columns) + 2]
    tables, ghost, staged, own, acc, turned = refs[len(columns) + 2 :]
    pad = columns[0].shape[0] // 3
    lam = coupling[0]
    types = sigma_t.shape[1]
    tables[0, :, 0:types] = jnp.broadcast_to(0.5 * sigma_t[...], (SUB, types))
    tables[1, :, 0:types] = jnp.broadcast_to(2.0 * jnp.sqrt(depth_t[...]), (SUB, types))
    tables[2, :, 0:types] = jnp.broadcast_to(charge_t[...], (SUB, types))
    for column in range(len(columns)):
        for a in range(3):
            part = [
                columns[column][a * pad + k * blocks : a * pad + k * blocks + SUB, :]
                for k in range(5)
            ]
            kind = part[3].astype(jnp.int32)
            fixed = [gather_lanes(tables[t], kind) for t in range(3)] + [part[4]]
            for where, (b, c) in images:
                if where != column:
                    continue
                at = (9 * a + 3 * b + c) * blocks
                for dim, step in enumerate((a, b, c)):
                    spot = (part[dim] + float(step - 1)) * edge[dim] * spacing
                    ghost[dim, at : at + blocks, :] = spot[0:blocks]
                for t in range(4):
                    ghost[3 + t, at : at + blocks, :] = fixed[t][0:blocks]
    centre = 13 * blocks
    staged[...] = jnp.zeros(staged.shape, jnp.float32)
    for k in range(7):
        staged[SUB * k : SUB * k + blocks, :] = ghost[k, centre : centre + blocks, :]
    columns_of = staged[...].T
    for q in range(blocks):
        for k in range(7):
            lane = SUB * k + q
            spread = jnp.broadcast_to(columns_of[:, lane : lane + 1], (LANES, LANES))
            if k == 5:
                spread = spread * coulomb
            own[q, k] = spread
            if k == 6:
                own[q, 7] = soft_base + soft_alpha * (lam * spread)
                own[q, 8] = 1.0 - lam * spread
    own_flag = staged[6 * SUB : 7 * SUB, :]
    own_eps = staged[4 * SUB : 5 * SUB, :]
    own_charge = staged[5 * SUB : 6 * SUB, :]
    self_a = soft_base + soft_alpha * (lam * own_flag)
    self_u = 1.0 / self_a
    self_t = own_eps * own_eps * self_u
    self_tu = self_t * self_u
    self_lj = self_tu - self_t
    self_rs = lax.rsqrt(self_a)
    self_c = coulomb * own_charge * own_charge * self_rs
    self_v = self_lj + self_c
    self_g = (self_lj + self_tu) * self_u + 0.5 * (self_c * (self_rs * self_rs))
    self_pv = own_flag * self_v
    self_pg = own_flag * self_g
    row = lax.broadcasted_iota(jnp.int32, (SUB, LANES), 0)
    lane_full = lax.broadcasted_iota(jnp.int32, (LANES, LANES), 1)
    turned[...] = jnp.zeros(turned.shape, jnp.float32)
    slots = listed.shape[0] // blocks

    def block(q, totals):
        acc[...] = jnp.zeros(acc.shape, jnp.float32)

        def entry(e, carry):
            sum_v, sum_pv, sum_pg, selves = carry
            h = listed[q * slots + e]
            other = [
                jnp.broadcast_to(ghost[k, pl.ds(h, 1), :], (SUB, LANES)) for k in range(7)
            ]
            other_a = soft_base + soft_alpha * (lam * other[6])
            other_w = 1.0 - lam * other[6]
            for g in range(LANES // SUB):
                at = slice(g * SUB, g * SUB + SUB)
                dx = own[q, 0, at, :] - other[0]
                dy = own[q, 1, at, :] - other[1]
                dz = own[q, 2, at, :] - other[2]
                r2 = dx * dx + dy * dy + dz * dz
                sigma = own[q, 3, at, :] + other[3]
                eps4 = own[q, 4, at, :] * other[4]
                qq = own[q, 5, at, :] * other[5]
                p = jnp.maximum(own[q, 6, at, :], other[6])
                a = jnp.maximum(own[q, 7, at, :], other_a)
                w = jnp.minimum(own[q, 8, at, :], other_w)
                s2 = sigma * sigma
                s6 = s2 * s2 * s2
                r4 = r2 * r2
                inv = newton_reciprocal(s6 * a + r4 * r2)
                rs = lax.rsqrt(a + r2)
                u = s6 * inv
                t = eps4 * u
                tu = t * u
                lj = tu - t
                k = lj + tu
                vc = qq * rs
                vcr = vc * (rs * rs)
                f = w * (vcr + 6.0 * (k * (r4 * inv)))
                acc[0, at, :] += f * dx
                acc[1, at, :] += f * dy
                acc[2, at, :] += f * dz
                v = lj + vc
                sum_v = sum_v + v
                sum_pv = sum_pv + p * v
                sum_pg = sum_pg + p * (k * u + 0.5 * vcr)
            return sum_v, sum_pv, sum_pg, selves + jnp.where(h == centre + q, 1.0, 0.0)

        sum_v, sum_pv, sum_pg, selves = lax.fori_loop(
            0, counts[q], entry, totals + (jnp.float32(0.0),)
        )
        held = jnp.where(row == q, selves, 0.0)
        for k in range(3):
            total = jnp.sum(acc[k], axis=1, keepdims=True)
            turned[...] = jnp.where(lane_full == k * blocks + q, total, turned[...])
        return (
            sum_v - held * self_v,
            sum_pv - held * self_pv,
            sum_pg - held * self_pg,
        )

    zero = jnp.zeros((SUB, LANES), jnp.float32)
    sum_v, sum_pv, sum_pg = lax.fori_loop(0, blocks, block, (zero, zero, zero))
    forces[...] = turned[...].T[0 : 3 * blocks, :]
    energy = sum_v - lam * sum_pv
    dhdl = -sum_pv - 0.5 * (1.0 - lam) * sum_pg
    energy = jnp.sum(jnp.sum(energy, axis=0, keepdims=True), axis=1, keepdims=True)
    dhdl = jnp.sum(jnp.sum(dhdl, axis=0, keepdims=True), axis=1, keepdims=True)
    lane = lax.broadcasted_iota(jnp.int32, (1, LANES), 1)
    sums[...] = jnp.where(lane == 0, energy, jnp.where(lane == 1, dhdl, 0.0))


def summed(value, axis):
    count = lax.axis_size(axis)
    if count & (count - 1):
        return lax.psum(value, axis)
    step = 1
    while step < count:
        value = value + lax.ppermute(value, axis, [(i, i ^ step) for i in range(count)])
        step *= 2
    return value


def on_device(
    fraction,
    atom_type,
    perturbed,
    leaving,
    neighbours,
    counts,
    sigma_table,
    depth_table,
    charge_table,
    domain_edge,
    coupling,
):
    atom_count = fraction.shape[-1]
    blocks = atom_count // LANES
    spacing = float(atom_count) ** (1.0 / 3.0)
    mig = leaving.shape[-1]
    types = sigma_table.shape[0]
    count_x, count_y, count_z = (lax.axis_size(axis) for axis in ("dx", "dy", "dz"))
    pad = -(-(5 * blocks + 2) // SUB) * SUB
    vmem = pl.BlockSpec(memory_space=pltpu.VMEM)
    smem = pl.BlockSpec(memory_space=pltpu.SMEM)
    packed = pl.pallas_call(
        functools.partial(pack_kernel, blocks, 2 * mig),
        in_specs=[vmem] * 4,
        out_specs=vmem,
        out_shape=jax.ShapeDtypeStruct((pad + 2 * SUB, LANES), jnp.float32),
        scratch_shapes=[pltpu.VMEM((pad + 2 * SUB, LANES), jnp.float32)],
        name="pack",
    )(
        fraction.reshape(3 * blocks, LANES),
        atom_type.reshape(blocks, LANES),
        perturbed.reshape(blocks, LANES),
        leaving.reshape(1, 2 * mig),
    )
    below = lax.ppermute(packed, "dx", ring(count_x, -1))
    above = lax.ppermute(packed, "dx", ring(count_x, 1))
    leavers = packed[pad + SUB :]
    below2 = lax.ppermute(leavers, "dx", ring(count_x, -2))
    if (count_x - 2) % count_x == 2 % count_x:
        above2 = below2
    else:
        above2 = lax.ppermute(leavers, "dx", ring(count_x, 2))
    moved = pl.pallas_call(
        functools.partial(migrate_kernel, blocks, mig),
        in_specs=[vmem] * 5,
        out_specs=vmem,
        out_shape=jax.ShapeDtypeStruct((3 * pad, LANES), jnp.float32),
        name="migrate",
    )(below2, below, packed, above, above2)
    places, columns, images = {(0, 0): 0}, [moved], []
    for b in range(3):
        for c in range(3):
            key = ((b - 1) % count_y, (c - 1) % count_z)
            if key not in places:
                places[key] = len(columns)
                columns.append(
                    lax.ppermute(moved, ("dy", "dz"), grid_ring(count_y, count_z, *key))
                )
            images.append((places[key], (b, c)))
    rows = -(-27 * blocks // SUB) * SUB
    forces, sums = pl.pallas_call(
        functools.partial(pair_kernel, blocks, spacing, images),
        in_specs=[smem] * 4 + [vmem] * (3 + len(columns)),
        out_specs=[vmem, vmem],
        out_shape=[
            jax.ShapeDtypeStruct((3 * blocks, LANES), jnp.float32),
            jax.ShapeDtypeStruct((1, LANES), jnp.float32),
        ],
        scratch_shapes=[
            pltpu.VMEM((3, SUB, LANES), jnp.float32),
            pltpu.VMEM((7, rows, LANES), jnp.float32),
            pltpu.VMEM((LANES, LANES), jnp.float32),
            pltpu.VMEM((blocks, 9, LANES, LANES), jnp.float32),
            pltpu.VMEM((3, LANES, LANES), jnp.float32),
            pltpu.VMEM((LANES, LANES), jnp.float32),
        ],
        name="pairs",
    )(
        neighbours.reshape(-1),
        counts.reshape(-1),
        domain_edge,
        coupling,
        sigma_table.reshape(1, types),
        depth_table.reshape(1, types),
        charge_table.reshape(1, types),
        *columns,
    )
    forces = forces.reshape(3, 1, 1, 1, atom_count)
    for axis in ("dz", "dy", "dx"):
        sums = summed(sums, axis)
    sums = sums * (0.5 / (atom_count * count_x * count_y * count_z))
    return (forces, sums[0, 0:1], sums[0, 1:2])


def solution(mesh):
    return jax.shard_map(
        on_device,
        mesh=mesh,
        in_specs=(
            P(None, ("win", "dx"), "dy", "dz", None),
            P(("win", "dx"), "dy", "dz", None),
            P(("win", "dx"), "dy", "dz", None),
            P(("win", "dx"), "dy", "dz", None, None),
            P(("win", "dx"), "dy", "dz", None, None),
            P(("win", "dx"), "dy", "dz", None),
            P(),
            P(),
            P(),
            P(),
            P("win"),
        ),
        out_specs=(P(None, ("win", "dx"), "dy", "dz", None), P("win"), P("win")),
        check_vma=False,
    )
```

```python
import functools

import jax
import jax.numpy as jnp
from jax import lax
from jax.experimental import pallas as pl
from jax.experimental.pallas import tpu as pltpu
from jax.sharding import PartitionSpec as P

soft_base = 0.3
soft_alpha = 0.5
charge_base = 0.3
charge_alpha = 0.5
coulomb = 0.1
LANES = 128
SUB = 8


def ring(count, by):
    return [((i + by) % count, i) for i in range(count)]


def grid_ring(count_y, count_z, by_y, by_z):
    route = []
    for y in range(count_y):
        for z in range(count_z):
            source = ((y + by_y) % count_y) * count_z + (z + by_z) % count_z
            route.append((source, y * count_z + z))
    return route


def near(array):
    return pltpu.with_memory_space_constraint(array, pltpu.VMEM)


def gather_lanes(rows, lanes):
    return jnp.take_along_axis(rows, lanes, axis=1, mode="promise_in_bounds")


def pack_kernel(
    blocks, fraction, kind, flag, leaving, sigma_t, depth_t, charge_t, out, leavers, tables
):
    tables[...] = jnp.zeros(tables.shape, jnp.float32)
    type_rows(tables, sigma_t, depth_t, charge_t)
    mig = leaving.shape[-1]
    head = out.shape[0] - 2 * SUB
    out[5 * blocks :, :] = jnp.zeros((out.shape[0] - 5 * blocks, LANES), jnp.float32)
    for q in range(blocks):
        part = slice(q * LANES, q * LANES + LANES)
        for k in range(3):
            out[k * blocks + q : k * blocks + q + 1, :] = fraction[k, 0, 0, :, part]
        at = 3 * blocks + q
        out[at : at + 1, :] = kind[0, 0, :, part].astype(jnp.float32)
        at = 4 * blocks + q
        out[at : at + 1, :] = flag[0, 0, :, part].astype(jnp.float32)
    for side in range(2):
        out[head : head + 1, side * mig : side * mig + mig] = leaving[
            0, 0, 0, side : side + 1, :
        ].astype(jnp.float32)
    slots = jnp.broadcast_to(out[head : head + 1, :], (SUB, LANES)).astype(jnp.int32)
    lane = slots & (LANES - 1)
    here = lax.broadcasted_iota(jnp.int32, (SUB, LANES), 0) == (slots >> 7)
    for k in range(5):
        picked = gather_lanes(out[k * blocks : k * blocks + SUB, :], lane)
        picked = jnp.sum(jnp.where(here, picked, 0.0), axis=0, keepdims=True)
        at = head + SUB + k
        out[at : at + 1, :] = picked
    leavers[...] = out[head + SUB :, :]


def migrate_kernel(blocks, mig, below2, below, own, above, above2, out):
    pad = own.shape[0] - 2 * SUB
    tail = pad + SUB
    leavers = [
        below2[...],
        below[tail : tail + SUB, :],
        own[tail : tail + SUB, :],
        above[tail : tail + SUB, :],
        above2[...],
    ]
    lane = lax.broadcasted_iota(jnp.int32, (SUB, LANES), 1)
    row = lax.broadcasted_iota(jnp.int32, (SUB, LANES), 0)
    place = row * LANES + lane
    shift = jnp.where(row == 0, 1.0, 0.0)
    for d, base in enumerate((below, own, above)):
        slots = jnp.broadcast_to(base[pad : pad + 1, :], (SUB, LANES)).astype(jnp.int32)
        from_above = pltpu.roll(leavers[d + 2], LANES - mig, 1) + shift
        from_below = pltpu.roll(leavers[d], mig, 1) - shift
        incoming = jnp.where(lane < mig, from_above, from_below)
        origin = jnp.full((SUB, LANES), -1, jnp.int32)
        for m in range(2 * mig):
            spot = jnp.broadcast_to(slots[:, m : m + 1], (SUB, LANES))
            origin = jnp.where(place == spot, m, origin)
        arrives = origin >= 0
        source = jnp.maximum(origin, 0)
        for k in range(5):
            fresh = gather_lanes(jnp.broadcast_to(incoming[k : k + 1, :], (SUB, LANES)), source)
            held = base[k * blocks : k * blocks + SUB, :]
            kept = jnp.where(arrives, fresh, held)
            start = d * pad + k * blocks
            out[start : start + blocks, :] = kept[0:blocks]


def type_rows(tables, sigma_t, depth_t, charge_t):
    types = sigma_t.shape[1]
    tables[0, :, 0:types] = jnp.broadcast_to(0.5 * sigma_t[...], (SUB, types))
    tables[1, :, 0:types] = jnp.broadcast_to(2.0 * jnp.sqrt(depth_t[...]), (SUB, types))
    tables[2, :, 0:types] = jnp.broadcast_to(charge_t[...], (SUB, types))


def domain_rows(column, a, blocks, tables):
    pad = column.shape[0] // 3
    part = [column[a * pad + k * blocks : a * pad + k * blocks + SUB, :] for k in range(5)]
    kind = part[3].astype(jnp.int32)
    return part[0:3], [gather_lanes(tables[t], kind) for t in range(3)] + [part[4]]


def positions(spots, steps, edge, spacing):
    return [
        (spot + float(step - 1)) * edge[dim] * spacing
        for dim, (spot, step) in enumerate(zip(spots, steps))
    ]


def spread_kernel(
    blocks, spacing, edge, coupling, tables, moved, own, selves, staged
):
    lam = coupling[0]
    spots, fixed = domain_rows(moved, 1, blocks, tables)
    rows = positions(spots, (1, 1, 1), edge, spacing) + fixed
    staged[...] = jnp.zeros(staged.shape, jnp.float32)
    for k in range(7):
        staged[SUB * k : SUB * k + blocks, :] = rows[k][0:blocks]
    flag, eps, charge = rows[6], rows[4], rows[5]
    a = soft_base + soft_alpha * (lam * flag)
    u = 1.0 / a
    t = eps * eps * u
    tu = t * u
    lj = tu - t
    rs = lax.rsqrt(a)
    vc = coulomb * charge * charge * rs
    v = lj + vc
    real = lax.broadcasted_iota(jnp.int32, (SUB, LANES), 0) < blocks
    selves[0] = jnp.where(real, v, 0.0)
    selves[1] = jnp.where(real, flag * v, 0.0)
    selves[2] = jnp.where(real, flag * ((lj + tu) * u + 0.5 * (vc * (rs * rs))), 0.0)
    columns_of = staged[...].T
    for q in range(blocks):
        for k in range(7):
            lane = SUB * k + q
            spread = jnp.broadcast_to(columns_of[:, lane : lane + 1], (LANES, LANES))
            if k == 5:
                spread = spread * coulomb
            own[q, k] = spread
            if k == 6:
                own[q, 7] = soft_base + soft_alpha * (lam * spread)
                own[q, 8] = 1.0 - lam * spread


def pair_kernel(
    blocks, spacing, images, listed, counts, edge, coupling, tables, own, selves, *refs
):
    columns = refs[: max(c for c, _ in images) + 1]
    acc, sums = refs[len(columns) : len(columns) + 2]
    (ghost,) = refs[len(columns) + 2 :]
    lam = coupling[0]
    for column in range(len(columns)):
        for a in range(3):
            spots, fixed = domain_rows(columns[column], a, blocks, tables)
            for where, (b, c) in images:
                if where != column:
                    continue
                at = (9 * a + 3 * b + c) * blocks
                rows = positions(spots, (a, b, c), edge, spacing) + fixed
                for k in range(7):
                    ghost[k, at : at + blocks, :] = rows[k][0:blocks]
    centre = 13 * blocks
    row = lax.broadcasted_iota(jnp.int32, (SUB, LANES), 0)
    slots = listed.shape[0] // blocks

    def block(q, totals):
        acc[q] = jnp.zeros(acc.shape[1:], jnp.float32)

        def entry(e, carry):
            sum_v, sum_pv, sum_pg, itself = carry
            h = listed[q * slots + e]
            other = [
                jnp.broadcast_to(ghost[k, pl.ds(h, 1), :], (SUB, LANES)) for k in range(7)
            ]
            other_a = soft_base + soft_alpha * (lam * other[6])
            other_w = 1.0 - lam * other[6]
            for g in range(LANES // SUB):
                at = slice(g * SUB, g * SUB + SUB)
                dx = own[q, 0, at, :] - other[0]
                dy = own[q, 1, at, :] - other[1]
                dz = own[q, 2, at, :] - other[2]
                r2 = dx * dx + dy * dy + dz * dz
                sigma = own[q, 3, at, :] + other[3]
                eps4 = own[q, 4, at, :] * other[4]
                qq = own[q, 5, at, :] * other[5]
                p = jnp.maximum(own[q, 6, at, :], other[6])
                a = jnp.maximum(own[q, 7, at, :], other_a)
                w = jnp.minimum(own[q, 8, at, :], other_w)
                s2 = sigma * sigma
                s6 = s2 * s2 * s2
                r4 = r2 * r2
                root = lax.rsqrt(s6 * a + r4 * r2)
                inv = root * root
                rs = lax.rsqrt(a + r2)
                u = s6 * inv
                t = eps4 * u
                tu = t * u
                lj = tu - t
                k = lj + tu
                vc = qq * rs
                vcr = vc * (rs * rs)
                f = w * (vcr + 6.0 * (k * (r4 * inv)))
                acc[q, 0, at, :] += f * dx
                acc[q, 1, at, :] += f * dy
                acc[q, 2, at, :] += f * dz
                v = lj + vc
                sum_v = sum_v + v
                sum_pv = sum_pv + p * v
                sum_pg = sum_pg + p * (k * u + 0.5 * vcr)
            return sum_v, sum_pv, sum_pg, itself + jnp.where(h == centre + q, 1.0, 0.0)

        *sums_of, itself = lax.fori_loop(0, counts[q], entry, totals + (jnp.float32(0.0),))
        held = jnp.where(row == q, itself, 0.0)
        return tuple(total - held * selves[k] for k, total in enumerate(sums_of))

    zero = jnp.zeros((SUB, LANES), jnp.float32)
    sum_v, sum_pv, sum_pg = lax.fori_loop(0, blocks, block, (zero, zero, zero))
    energy = sum_v - lam * sum_pv
    dhdl = -sum_pv - 0.5 * (1.0 - lam) * sum_pg
    energy = jnp.sum(jnp.sum(energy, axis=0, keepdims=True), axis=1, keepdims=True)
    dhdl = jnp.sum(jnp.sum(dhdl, axis=0, keepdims=True), axis=1, keepdims=True)
    lane = lax.broadcasted_iota(jnp.int32, (1, LANES), 1)
    sums[...] = jnp.where(lane == 0, energy, jnp.where(lane == 1, dhdl, 0.0))


def finish_kernel(blocks, acc, forces, turned):
    lane = lax.broadcasted_iota(jnp.int32, (LANES, LANES), 1)
    held = jnp.zeros((LANES, LANES), jnp.float32)
    for q in range(blocks):
        for k in range(3):
            total = jnp.sum(acc[q, k], axis=1, keepdims=True)
            held = jnp.where(lane == k * blocks + q, total, held)
    turned[...] = held.T
    for k in range(3):
        for q in range(blocks):
            at = k * blocks + q
            forces[k, 0, 0, :, q * LANES : q * LANES + LANES] = turned[at : at + 1, :]


def summed(value, axis):
    count = lax.axis_size(axis)
    if count & (count - 1):
        return lax.psum(value, axis)
    step = 1
    while step < count:
        value = value + lax.ppermute(value, axis, [(i, i ^ step) for i in range(count)])
        step *= 2
    return value


def on_device(
    fraction,
    atom_type,
    perturbed,
    leaving,
    neighbours,
    counts,
    sigma_table,
    depth_table,
    charge_table,
    domain_edge,
    coupling,
):
    atom_count = fraction.shape[-1]
    blocks = atom_count // LANES
    spacing = float(atom_count) ** (1.0 / 3.0)
    mig = leaving.shape[-1]
    types = sigma_table.shape[0]
    count_x, count_y, count_z = (lax.axis_size(axis) for axis in ("dx", "dy", "dz"))
    pad = -(-(5 * blocks) // SUB) * SUB
    vmem = pl.BlockSpec(memory_space=pltpu.VMEM)
    smem = pl.BlockSpec(memory_space=pltpu.SMEM)
    packed, leavers, tables = pl.pallas_call(
        functools.partial(pack_kernel, blocks),
        in_specs=[vmem] * 7,
        out_specs=[vmem] * 3,
        out_shape=[
            pltpu.VMEM((pad + 2 * SUB, LANES), jnp.float32),
            pltpu.VMEM((SUB, LANES), jnp.float32),
            pltpu.VMEM((3, SUB, LANES), jnp.float32),
        ],
        name="pack",
    )(
        fraction,
        atom_type,
        perturbed,
        leaving,
        *(table.reshape(1, types) for table in (sigma_table, depth_table, charge_table)),
    )
    below = lax.ppermute(packed, "dx", ring(count_x, -1))
    above = lax.ppermute(packed, "dx", ring(count_x, 1))
    below2 = lax.ppermute(leavers, "dx", ring(count_x, -2))
    if (count_x - 2) % count_x == 2 % count_x:
        above2 = below2
    else:
        above2 = lax.ppermute(leavers, "dx", ring(count_x, 2))
    moved = pl.pallas_call(
        functools.partial(migrate_kernel, blocks, mig),
        in_specs=[vmem] * 5,
        out_specs=vmem,
        out_shape=pltpu.VMEM((3 * pad, LANES), jnp.float32),
        name="migrate",
    )(*(near(part) for part in (below2, below, packed, above, above2)))
    places, columns, images = {(0, 0): 0}, [moved], []
    for b in range(3):
        for c in range(3):
            key = ((b - 1) % count_y, (c - 1) % count_z)
            if key not in places:
                places[key] = len(columns)
                columns.append(
                    lax.ppermute(moved, ("dy", "dz"), grid_ring(count_y, count_z, *key))
                )
            images.append((places[key], (b, c)))
    rows = -(-27 * blocks // SUB) * SUB
    own, selves = pl.pallas_call(
        functools.partial(spread_kernel, blocks, spacing),
        in_specs=[smem] * 2 + [vmem] * 2,
        out_specs=[vmem, vmem],
        out_shape=[
            pltpu.VMEM((blocks, 9, LANES, LANES), jnp.float32),
            pltpu.VMEM((3, SUB, LANES), jnp.float32),
        ],
        scratch_shapes=[pltpu.VMEM((LANES, LANES), jnp.float32)],
        cost_estimate=pl.CostEstimate(flops=4000000, bytes_accessed=0, transcendentals=0),
        compiler_params=pltpu.CompilerParams(vmem_limit_bytes=8 << 20),
        name="spread",
    )(domain_edge, coupling, near(tables), near(moved))
    acc, sums = pl.pallas_call(
        functools.partial(pair_kernel, blocks, spacing, images),
        in_specs=[smem] * 4 + [vmem] * (3 + len(columns)),
        out_specs=[vmem, vmem],
        out_shape=[
            pltpu.VMEM((blocks, 3, LANES, LANES), jnp.float32),
            pltpu.VMEM((1, LANES), jnp.float32),
        ],
        scratch_shapes=[
            pltpu.VMEM((7, rows, LANES), jnp.float32),
        ],
        compiler_params=pltpu.CompilerParams(vmem_limit_bytes=8 << 20),
        name="pairs",
    )(
        neighbours.reshape(-1),
        counts.reshape(-1),
        domain_edge,
        coupling,
        near(tables),
        near(own),
        near(selves),
        *(near(part) for part in columns),
    )
    forces = pl.pallas_call(
        functools.partial(finish_kernel, blocks),
        in_specs=[vmem],
        out_specs=vmem,
        out_shape=jax.ShapeDtypeStruct(fraction.shape, jnp.float32),
        scratch_shapes=[pltpu.VMEM((LANES, LANES), jnp.float32)],
        cost_estimate=pl.CostEstimate(flops=4000000, bytes_accessed=0, transcendentals=0),
        compiler_params=pltpu.CompilerParams(vmem_limit_bytes=8 << 20),
        name="finish",
    )(near(acc))
    for axis in ("dz", "dy", "dx"):
        sums = summed(sums, axis)
    sums = sums * (0.5 / (atom_count * count_x * count_y * count_z))
    return (forces, sums[0, 0:1], sums[0, 1:2])


def solution(mesh):
    return jax.shard_map(
        on_device,
        mesh=mesh,
        in_specs=(
            P(None, ("win", "dx"), "dy", "dz", None),
            P(("win", "dx"), "dy", "dz", None),
            P(("win", "dx"), "dy", "dz", None),
            P(("win", "dx"), "dy", "dz", None, None),
            P(("win", "dx"), "dy", "dz", None, None),
            P(("win", "dx"), "dy", "dz", None),
            P(),
            P(),
            P(),
            P(),
            P("win"),
        ),
        out_specs=(P(None, ("win", "dx"), "dy", "dz", None), P("win"), P("win")),
        check_vma=False,
    )
```
